16 devices in a mesh: rep: 2 (over y, z), dp: 8 (over x, core).
Axes of the slice: x: 4, y: 2, z: 1, core: 2. Of those that a mesh axis runs over, the one named last changes fastest.
The devices are a block of a 4x4x8 slice.
Arguments:
- x: bfloat16 [16, 2048, 896], P(('rep', 'dp')), parts along dimension 0
- dy: bfloat16 [16, 2048, 896], P(('rep', 'dp')), parts along dimension 0
- w_gate: bfloat16 [2, 896, 2560], P(None, 'dp')
- w_up: bfloat16 [2, 896, 2560], P(None, 'dp')
- w_down: bfloat16 [2, 2560, 896], P(None, 'dp')
- m_w_gate: float32 [2, 896, 2560], P(None, 'dp')
- m_w_up: float32 [2, 896, 2560], P(None, 'dp')
- m_w_down: float32 [2, 2560, 896], P(None, 'dp')
- v_w_gate: float32 [2, 896, 2560], P(None, 'dp')
- v_w_up: float32 [2, 896, 2560], P(None, 'dp')
- v_w_down: float32 [2, 2560, 896], P(None, 'dp')
Outputs:
- output 1: bfloat16 [4, 896, 2560], P('rep', 'dp'), parts along dimension 0
- output 2: bfloat16 [4, 896, 2560], P('rep', 'dp'), parts along dimension 0
- output 3: bfloat16 [4, 2560, 896], P('rep', 'dp'), parts along dimension 0
- output 4: float32 [4, 896, 2560], P('rep', 'dp'), parts along dimension 0
- output 5: float32 [4, 896, 2560], P('rep', 'dp'), parts along dimension 0
- output 6: float32 [4, 2560, 896], P('rep', 'dp'), parts along dimension 0
- output 7: float32 [4, 896, 2560], P('rep', 'dp'), parts along dimension 0
- output 8: float32 [4, 896, 2560], P('rep', 'dp'), parts along dimension 0
- output 9: float32 [4, 2560, 896], P('rep', 'dp'), parts along dimension 0
There are 2 independent parts. The reference program is written for one: setup_inputs(seed, part) draws one part's arguments, and reference() takes and returns one part's arrays. A program takes and returns all parts, laid end to end along the dimension named above; an argument that names none is the same for every part.
All inputs are finite; a program needn't handle non-finite values.
Results may differ from the reference program's by a relative error of at most 0.022.
Values are sent between devices in bfloat16 or wider.
A program may use at most 768 MiB of HBM per device.

```python
import jax
import jax.numpy as jnp
from jax import lax

SEQUENCES = 8
TOKENS = 2048
D = 896
FF = 2560
LAYERS = 2
NAMES = ("w_gate", "w_up", "w_down")
SHAPES = {"w_gate": (LAYERS, D, FF), "w_up": (LAYERS, D, FF), "w_down": (LAYERS, FF, D)}


def bump(key, n, height):
    away = (jnp.arange(n, dtype=jnp.int32) - jax.random.randint(key, (), 0, n, jnp.int32)) % n
    return jnp.where(away < n // 8, height, 1.0)


def together(key, own, strength):
    shared = jax.random.normal(key, own.shape[1:], jnp.float32)
    return (own + strength * shared) * lax.rsqrt(1 + strength * strength)


def setup_inputs(seed: int = 0, part: int = 0) -> dict:
    kx, kdy, ka, kb, kz, kf, kh, kl, *keys = jax.random.split(jax.random.key(seed), 8 + 3 * len(NAMES))
    kx, kdy, ka, kb = (jax.random.fold_in(k, part) for k in (kx, kdy, ka, kb))
    kw, km, kv = (keys[i::3] for i in range(3))
    shape = (SEQUENCES, TOKENS, D)
    much_x, much_dy = jax.random.uniform(kz, (2,), jnp.float32, 0.0, 1.0)
    loud = 2.0 ** jax.random.uniform(jax.random.fold_in(kz, 1), (), jnp.float32, -1.0, 2.0)
    layers = 2.0 ** jax.random.uniform(kl, (LAYERS, 1, 1), jnp.float32, -1.0, 1.0)
    x = together(ka, jax.random.normal(kx, shape, jnp.float32), much_x) * bump(kf, D, 4.0)
    dy = together(kb, jax.random.normal(kdy, shape, jnp.float32), much_dy)
    drawn = {"x": x.astype(jnp.bfloat16), "dy": (loud * dy * (SEQUENCES * TOKENS) ** -0.5).astype(jnp.bfloat16)}
    for key, name in zip(kw, NAMES, strict=True):
        w = jax.random.normal(key, SHAPES[name], jnp.float32) * SHAPES[name][1] ** -0.5
        drawn[name] = (w * {"w_gate": 1.0, "w_up": bump(kh, FF, 4.0), "w_down": layers}[name]).astype(jnp.bfloat16)
    for key, name in zip(km, NAMES, strict=True):
        drawn[f"m_{name}"] = 0.1 * jax.random.normal(key, SHAPES[name], jnp.float32)
    for key, name in zip(kv, NAMES, strict=True):
        drawn[f"v_{name}"] = jax.random.uniform(key, SHAPES[name], jnp.float32, 0.005, 0.015)
    return drawn


def matmul(a, w):
    return jnp.dot(a, w, preferred_element_type=jnp.float32).astype(jnp.bfloat16)


def normed(h):
    wide = h.astype(jnp.float32)
    scale = lax.rsqrt(jnp.mean(wide**2, -1, keepdims=True) + 1e-6)
    return (wide * scale).astype(jnp.bfloat16)


def layer(h, w):
    a = normed(h)
    gate = jnp.dot(a, w["w_gate"], preferred_element_type=jnp.float32)
    up = jnp.dot(a, w["w_up"], preferred_element_type=jnp.float32)
    return h + matmul((jax.nn.silu(gate) * up).astype(jnp.bfloat16), w["w_down"])


def adamw(w, m, v, g):
    m = 0.9 * m + 0.1 * g
    v = 0.95 * v + 0.05 * g * g
    step = m * lax.rsqrt(v + 1e-8) + 0.1 * w
    return (w - 0.02 * step).astype(jnp.bfloat16), m, v


def clipped(gradients, sum_of_squares, count):
    factor = jnp.minimum(1.0, 0.5 * lax.rsqrt(sum_of_squares / count + 1e-30))
    return [g * factor for g in gradients]


def stack(weights, h):
    return lax.scan(lambda h, w: (layer(h, w), None), h, weights)[0]


def reference(x, dy, w_gate, w_up, w_down, m_w_gate, m_w_up, m_w_down, v_w_gate, v_w_up, v_w_down):
    weights = dict(zip(NAMES, (w_gate, w_up, w_down), strict=True))

    def take(so_far, sequence):
        h, by_y = sequence
        _, back = jax.vjp(lambda w: stack(w, h), weights)
        return jax.tree.map(lambda total, term: total + term.astype(jnp.float32), so_far, back(by_y)[0]), None

    none_yet = {name: jnp.zeros(w.shape, jnp.float32) for name, w in weights.items()}
    by_weights, _ = lax.scan(take, none_yet, (x, dy))
    gradients = [by_weights[name].astype(jnp.bfloat16).astype(jnp.float32) for name in NAMES]
    gradients = clipped(gradients, sum(jnp.sum(g * g) for g in gradients), sum(g.size for g in gradients))
    new = [
        adamw(w.astype(jnp.float32), m, v, g)
        for w, m, v, g in zip((w_gate, w_up, w_down), (m_w_gate, m_w_up, m_w_down), (v_w_gate, v_w_up, v_w_down), gradients, strict=True)
    ]
    return tuple(one[which] for which in range(3) for one in new)
```

```python
import functools

import jax
import jax.numpy as jnp
from jax import lax
from jax.experimental import pallas as pl
from jax.experimental.pallas import tpu as pltpu
from jax.sharding import PartitionSpec as P

MESH = pl.DeviceIdType.MESH
BF, F32 = jnp.bfloat16, jnp.float32
CH = 512
SUB = 256
VMEM_LIMIT = 67_043_328
FIRST, SECOND, ALL = 0, 1, None


def dot(a, b, ca, cb):
    return lax.dot_general(a, b, (((ca,), (cb,)), ((), ())), preferred_element_type=F32)


nn = functools.partial(dot, ca=1, cb=0)
nt = functools.partial(dot, ca=1, cb=1)
tn = functools.partial(dot, ca=0, cb=0)


def place():
    me = lax.axis_index("dp")
    x, k = me // 2, me % 2
    chips = (x, x + 1 - 2 * (x % 2), (x + 2) % 4, 3 - x)
    return me, k, chips, [2 * c + k for c in chips], [2 * c + 1 - k for c in chips]


def meet(devices):
    barrier = pltpu.get_barrier_semaphore()
    for d in devices:
        pl.semaphore_signal(barrier, device_id={"dp": d}, device_id_type=MESH)
    pl.semaphore_wait(barrier, len(devices))


def remote(src, dst, send, recv, device):
    return pltpu.make_async_remote_copy(src_ref=src, dst_ref=dst, send_sem=send, recv_sem=recv, device_id={"dp": device}, device_id_type=MESH)


def when(condition, *acts):
    @pl.when(condition)
    def _():
        for act in acts:
            act()


def tile(t, size):
    return pl.ds(pl.multiple_of(t * size, size), size)


def lanes(start, size):
    return pl.ds(start if isinstance(start, int) else pl.multiple_of(start, 128), size)


class Local:
    def __init__(self, sems):
        self.sems, self.used = sems, 0

    def __call__(self, src, dst):
        copy = pltpu.make_async_copy(src, dst, self.sems.at[self.used])
        self.used += 1
        copy.start()
        return copy


def normed(h):
    wide = h.astype(F32)
    scale = lax.rsqrt(jnp.mean(wide * wide, -1, keepdims=True) + 1e-6)
    return (wide * scale).astype(BF)


def norm_rows(src, dst):
    @pl.loop(0, src.shape[0] // SUB)
    def _(t):
        dst[tile(t, SUB), :] = normed(src[tile(t, SUB), :])


def squares(g):
    g = g.astype(F32)
    return jnp.sum((g * g).reshape(-1, 8, g.shape[-1]), 0)


class Gather:
    def __init__(self, send, recv):
        self.send, self.recv = send, recv
        self.me, k, chips, (n0, n1, n2, n3), (o0, o1, o2, o3) = place()
        self.partners = (n1, n3, o0)
        self.moves = [
            (n0, ALL, n1), (n0, ALL, n3), (n0, ALL, o0), (n1, FIRST, n3), (n3, SECOND, n1),
            (n1, ALL, o0), (n3, ALL, o0), (n2, FIRST, o0), (n2, SECOND, o0),
        ]
        self.lands = [(n1, ALL), (n3, ALL), (o0, ALL), (n2, FIRST), (n2, SECOND), (o1, ALL), (o3, ALL), (o2, FIRST), (o2, SECOND)]

    def region(self, item, dev, half):
        src, layer, at, buf, blk, r0, rn, c0, cn, by_rows = item
        row = dev * blk + r0
        if half is not ALL:
            if by_rows:
                rn //= 2
                row = row + half * rn
            else:
                cn //= 2
                c0 = c0 + half * cn
        return buf.at[pl.ds(pl.multiple_of(row, 16), rn), lanes(c0, cn)]

    def nth(self, i, item, c):
        source, half, to = self.moves[c]
        src = dst = self.region(item, source, half)
        if source is self.moves[0][0]:
            array, layer, at, buf, blk, r0, rn, c0, cn, by_rows = item
            src = array.at[layer, pl.ds(r0, rn), lanes(at, cn)]
        return remote(src, dst, self.send.at[i, c], self.recv.at[i, c], to)

    def arrived(self, i, item, c):
        what = self.region(item, *self.lands[c])
        remote(what, what, self.send.at[i, c], self.recv.at[i, c], self.partners[0]).wait_recv()

    def issue(self, piece):
        for i, item in piece:
            for c in (0, 1, 2):
                self.nth(i, item, c).start()

    def forward(self, piece):
        for i, item in piece:
            for c in (0, 1):
                self.arrived(i, item, c)
                self.nth(i, item, c + 3).start()
                self.nth(i, item, c + 5).start()

    def pass_on(self, piece):
        for i, item in piece:
            for c in (3, 4):
                self.arrived(i, item, c)
                self.nth(i, item, c + 4).start()

    def complete(self, piece):
        for i, item in piece:
            for c in (2, 5, 6, 7, 8):
                self.arrived(i, item, c)

    def sent(self, piece):
        for i, item in piece:
            for c in range(len(self.moves)):
                self.nth(i, item, c).wait_send()


def pair(layer, r, weights, W, f):
    return [(2 * f + m, (w, layer, f * CH, W, r, 0, r, (2 * f + m) * CH, CH, False)) for m, w in enumerate(weights)]


def own_rows(keep, layer, r, weights, W, me):
    nf = W.shape[1] // (2 * CH)
    return [keep(w.at[layer, :, pl.ds(f * CH, CH)], W.at[tile(me, r), pl.ds((2 * f + m) * CH, CH)]) for m, w in enumerate(weights) for f in range(nf)]


def forward_kernel(x_ref, wg_ref, wu_ref, wd_ref, h1_ref, a0_ref, g0_ref, u0_ref, wd0_ref, wd1_ref,
                   X, A, ACT, W, WD, GS, US, local, save, send, recv):
    T, D = X.shape
    F = ACT.shape[1]
    TM = GS.shape[1]
    r, rd, nf, tiles = wg_ref.shape[1], wd_ref.shape[1], F // CH, T // TM
    g, keep = Gather(send, recv), Local(local)
    x_in = keep(x_ref, X)
    own = own_rows(keep, 0, r, (wg_ref, wu_ref), W, g.me)
    own += [keep(wd_ref.at[layer], to.at[tile(g.me, rd), :]) for layer, to in enumerate((WD, wd1_ref))]
    meet(g.partners)
    chunk = functools.partial(pair, 0, r, (wg_ref, wu_ref), W)
    rest = [
        [(2 * (nf + layer) + i, (wd_ref, layer, 0, buf, rd, i * (rd // 2), rd // 2, 0, D, True))]
        for layer, buf in enumerate((WD, wd1_ref)) for i in range(2)
    ]

    def on(act, p, condition=True):
        when(condition & (p < nf), lambda: act(chunk(p)))
        for i, piece in enumerate(rest):
            when(condition & (p == nf + i), lambda: act(piece))

    ahead = 2
    for p in range(ahead):
        g.issue(chunk(p))
    x_in.wait()
    norm_rows(X, A)
    out = [keep(A, a0_ref), own.pop()]
    for c in own:
        c.wait()
    for p in range(ahead):
        g.forward(chunk(p))
        g.issue(chunk(p + ahead))
    g.pass_on(chunk(0))

    def saving(f, t):
        rows, cols, slot = tile(t, TM), tile(f, CH), t % 2
        return [pltpu.make_async_copy(S.at[slot], ref.at[rows, cols], save.at[i, slot]) for i, (S, ref) in enumerate(((GS, g0_ref), (US, u0_ref)))]

    @pl.loop(0, nf)
    def _(f):
        g.complete(chunk(f))

        @pl.loop(0, tiles)
        def _(t):
            on(g.forward, f + 2, t == tiles // 2)
            on(g.issue, f + 4, t == tiles // 2)
            copies, slot = saving(f, t), t % 2
            when((t > 1) | (f > 0), *[c.wait for c in copies])
            for j in range(TM // SUB):
                rows, part = tile(t * (TM // SUB) + j, SUB), pl.ds(j * SUB, SUB)
                both = nn(A[rows, :], W[:, tile(f, 2 * CH)])
                gate, up = both[:, :CH], both[:, CH:]
                GS[slot, part, :] = gate
                US[slot, part, :] = up
                ACT[rows, tile(f, CH)] = (gate * jax.nn.sigmoid(gate) * up).astype(BF)
            for c in copies:
                c.start()

        on(g.pass_on, f + 1)

    first, below, *last = rest
    g.complete(first)
    g.forward(last[0])
    g.pass_on(below)
    g.complete(below)
    out.append(keep(WD, wd0_ref))

    @pl.loop(0, T // CH)
    def _(t):
        rows = tile(t, CH)
        X[rows, :] = (X[rows, :].astype(F32) + nn(ACT[rows, :], WD[...]).astype(BF).astype(F32)).astype(BF)
        when(t == 0, lambda: g.forward(last[1]))
        when(t == 1, lambda: g.pass_on(last[0]))
        when(t == 2, lambda: g.pass_on(last[1]))

    out.append(keep(X, h1_ref))
    for p in last:
        g.complete(p)
    for p in [chunk(f) for f in range(nf)] + rest:
        g.sent(p)
    for t in range(tiles - 2, tiles):
        out += saving(nf - 1, t)
    for c in out:
        c.wait()


class Scatter:
    def __init__(self, r, refs, G, SQ, outs, sems):
        self.outs, self.saves = outs, sems
        self.R, (self.DS, self.DR), (self.AS, self.AR), (self.BS, self.BR), (self.CS, self.CR), (self.ES, self.ER) = refs[0], *zip(refs[1:-1:2], refs[2:-1:2])
        self.r, self.sems, self.G, self.SQ = r, refs[-1], G, SQ
        self.me, self.k, self.chips, (n0, n1, n2, n3), (o0, *_) = place()
        self.routes = ((self.DS, self.DR, o0), (self.AS, self.AR, n1), (self.BS, self.BR, n3), (self.CS, self.CR, n3), (self.ES, self.ER, n1))

    @staticmethod
    def scratch(r):
        sent = [(4, r, 2 * CH), (2, r, CH), (2, r, CH), (r, CH), (r, CH)]
        shapes = [s for one in sent for s in (one, (2, *one))]
        return [pltpu.VMEM((2, 8 * r, 2 * CH), F32), *[pltpu.VMEM(s, BF) for s in shapes], pltpu.SemaphoreType.DMA((5, 3))]

    def cp(self, which, f):
        src, dst, dev = self.routes[which]
        return remote(src, dst.at[f % 2], self.sems.at[which, 0], self.sems.at[which, 1 + f % 2], dev)

    def rows(self, q, core):
        return pl.ds(pl.multiple_of((2 * self.chips[q] + core) * self.r, 16), self.r)

    def dot_and_send(self, f, a, b):
        R = self.R.at[f % 2]
        R[...] = tn(a, b)
        when(f > 0, self.cp(0, f).wait_send)
        for q in range(4):
            self.DS[q] = R[self.rows(q, 1 - self.k), :].astype(BF)
        self.cp(0, f).start()

    def halve(self, f):
        s, R = f % 2, self.R.at[f % 2]
        self.cp(0, f).wait_recv()
        when(f > 0, self.cp(1, f).wait_send, self.cp(2, f).wait_send)
        v = [R[self.rows(q, self.k), :] + self.DR[s, q].astype(F32) for q in range(4)]
        self.AS[0], self.AS[1] = v[1][:, :CH].astype(BF), v[2][:, :CH].astype(BF)
        self.BS[0], self.BS[1] = v[3][:, CH:].astype(BF), v[2][:, CH:].astype(BF)
        R[self.rows(0, self.k), :] = v[0]
        R[self.rows(1, self.k), CH:] = v[1][:, CH:]
        R[self.rows(3, self.k), :CH] = v[3][:, :CH]
        self.cp(1, f).start()
        self.cp(2, f).start()

    def quarter(self, f):
        s, R, mine = f % 2, self.R.at[f % 2], self.rows(0, self.k)
        for which in (1, 2):
            self.cp(which, f).wait_recv()
        when(f > 0, self.cp(3, f).wait_send, self.cp(4, f).wait_send)
        self.CS[...] = (R[self.rows(3, self.k), :CH] + self.AR[s, 1].astype(F32)).astype(BF)
        self.ES[...] = (R[self.rows(1, self.k), CH:] + self.BR[s, 1].astype(F32)).astype(BF)
        self.cp(3, f).start()
        self.cp(4, f).start()
        R[mine, :CH] += self.AR[s, 0].astype(F32)
        R[mine, CH:] += self.BR[s, 0].astype(F32)

    def finish(self, f):
        s = f % 2
        for which in (3, 4):
            self.cp(which, f).wait_recv()
        v = self.R[s, self.rows(0, self.k), :]
        for m, (part, last) in enumerate(((v[:, :CH], self.CR), (v[:, CH:], self.ER))):
            g = (part + last[s].astype(F32)).astype(BF)
            when(f > 1, self.saving(f, m).wait)
            self.G[s, m] = g
            self.saving(f, m).start()
            self.SQ[...] += squares(g)

    def saving(self, f, m):
        return pltpu.make_async_copy(self.G.at[f % 2, m], self.outs[m].at[:, tile(f, CH)], self.saves.at[m, f % 2])

    def drain(self, f):
        for which in range(len(self.routes)):
            self.cp(which, f).wait_send()
        for m in range(2):
            self.saving(f, m).wait()
            self.saving(f - 1, m).wait()


def swiglu_back(gate, up, dact):
    sig = jax.nn.sigmoid(gate)
    silu = gate * sig
    dact = dact.astype(F32)
    return (silu * up).astype(BF), (dact * up * (sig + silu * (1.0 - sig))).astype(BF), (dact * silu).astype(BF)


def last_kernel(h1_ref, dy_ref, wg_ref, wu_ref, wd1_ref, gg_ref, gu_ref, act1_ref, dh1_ref, sq_ref,
                A, DY, W, WD, DGU, ACT, G, SQ, local, save, gsem, send, recv, *scatter):
    T, D = A.shape
    F = W.shape[1] // 2
    TM = 4 * SUB
    r, nf, tiles = wg_ref.shape[1], F // CH, T // TM
    g, keep = Gather(send, recv), Local(local)
    s = Scatter(r, scatter, G, SQ, (gg_ref.at[1], gu_ref.at[1]), gsem)
    h_in, dy_in, wd_in = keep(h1_ref, A), keep(dy_ref, DY), keep(wd1_ref, WD)
    own = own_rows(keep, 1, r, (wg_ref, wu_ref), W, g.me)
    meet(g.partners)
    piece = functools.partial(pair, 1, r, (wg_ref, wu_ref), W)
    g.issue(piece(0))
    SQ[...] = jnp.zeros_like(SQ)
    h_in.wait()
    norm_rows(A, A)
    dy_in.wait()
    wd_in.wait()

    @pl.loop(0, T // CH)
    def _(t):
        rows = tile(t, CH)
        dact = nt(DY[rows, :], WD[...]).astype(BF)
        for f in range(nf):
            DGU[rows, pl.ds((2 * f + 1) * CH, CH)] = dact[:, f * CH : (f + 1) * CH]
        when(t == 0, lambda: g.forward(piece(0)), lambda: g.issue(piece(1)))
        when(t == 1, lambda: g.issue(piece(2)))
        when(t == 2, lambda: g.pass_on(piece(0)))

    for c in own:
        c.wait()

    def save_act(f):
        return pltpu.make_async_copy(ACT, act1_ref.at[:, tile(f, CH)], save.at[0])

    @pl.loop(0, nf)
    def _(f):
        cols = tile(f, 2 * CH)
        g.complete(piece(f))
        when(f > 0, lambda: save_act(f).wait())

        @pl.loop(0, tiles)
        def _(t):
            when((t == 0) & (f > 1), lambda: s.quarter(f - 2))
            when((t == 0) & (f + 1 < nf), lambda: g.forward(piece(f + 1)))
            when((t == 0) & (f + 3 < nf), lambda: g.issue(piece(f + 3)))
            when((t == 1) & (f > 0), lambda: s.halve(f - 1))
            for j in range(TM // SUB):
                rows = tile(t * (TM // SUB) + j, SUB)
                both = nn(A[rows, :], W[:, cols])
                ACT[rows, :], DGU[rows, tile(2 * f, CH)], DGU[rows, tile(2 * f + 1, CH)] = swiglu_back(both[:, :CH], both[:, CH:], DGU[rows, tile(2 * f + 1, CH)])

        save_act(f).start()
        when(f + 1 < nf, lambda: g.pass_on(piece(f + 1)))
        when(f > 1, lambda: s.finish(f - 2))
        s.dot_and_send(f, A[...], DGU[:, cols])

    save_act(nf - 1).wait()
    keep(h1_ref, A).wait()

    @pl.loop(0, T // CH)
    def _(t):
        rows = tile(t, CH)
        da = nt(DGU[rows, :], W[...]).astype(BF).astype(F32)
        wide = A[rows, :].astype(F32)
        scale = lax.rsqrt(jnp.mean(wide * wide, -1, keepdims=True) + 1e-6)
        back = (da * scale - wide * (scale * scale * scale * jnp.mean(da * wide, -1, keepdims=True))).astype(BF)
        DY[rows, :] = (DY[rows, :].astype(F32) + back.astype(F32)).astype(BF)
        when(t == 0, lambda: s.quarter(nf - 2), lambda: s.halve(nf - 1))
        when(t == 1, lambda: s.finish(nf - 2), lambda: s.quarter(nf - 1))
        when(t == 2, lambda: s.finish(nf - 1))

    out = [keep(DY, dh1_ref)]
    sq_ref[...] = jnp.full(sq_ref.shape, jnp.sum(SQ[...]), F32)
    for f in range(nf):
        g.sent(piece(f))
    s.drain(nf - 1)
    for c in out:
        c.wait()


class DownScatter:
    def __init__(self, rd, refs, GD, SQ):
        (self.PT, self.PD, self.DS, self.DR, self.S1, self.R1, self.S3, self.R3, self.Q1, self.Q3, self.sems) = refs
        self.rd, self.GD, self.SQ = rd, GD, SQ
        self.me, self.k, self.chips, (n0, n1, n2, n3), (self.partner, *_) = place()
        near = ((self.S1, self.R1, n1), (self.S3, self.R3, n3))
        self.routes = [(S.at[i], R.at[i], n) for S, R, n in near for i in range(2)] + [(self.S1.at[0], self.Q1, n1), (self.S3.at[0], self.Q3, n3)]
        h = rd // 2
        self.top, self.low = slice(0, h), slice(h, rd)

    @staticmethod
    def scratch(rd, D):
        V = pltpu.VMEM
        return [
            V((2 * rd, D), F32), V((3, rd, D), F32), V((rd, D), BF), V((4, rd, D), BF),
            *[V((2, rd // 2, D), BF)] * 4, *[V((rd // 2, D), BF)] * 2, pltpu.SemaphoreType.DMA((10, 2)),
        ]

    def columns(self, s):
        x, x1, x2, x3 = self.chips
        c = jnp.where(s == 0, x2, jnp.where(s == 1, x1, jnp.where(s == 2, x3, x)))
        return pl.ds(pl.multiple_of(c * 2 * self.rd, 128), 2 * self.rd)

    def swap(self, s):
        return remote(self.DS, self.DR.at[s], self.sems.at[s, 0], self.sems.at[s, 1], self.partner)

    def cp(self, which):
        src, dst, dev = self.routes[which]
        return remote(src, dst, self.sems.at[4 + which, 0], self.sems.at[4 + which, 1], dev)

    def compute(self, s, act, rhs):
        rd = self.rd
        self.PT[...] = tn(act[:, self.columns(s)], rhs[...])
        when(s > 0, lambda: self.swap(s - 1).wait_send())
        self.PD[s % 3] = self.PT[tile(self.k, rd), :]
        self.DS[...] = self.PT[tile(1 - self.k, rd), :].astype(BF)
        self.swap(s).start()

    def halve(self, step):
        T, L = self.top, self.low
        self.swap(step).wait_recv()
        v = self.PD[step % 3] + self.DR[step].astype(F32)
        if step == 0:
            self.S1[0], self.S3[0] = v[T].astype(BF), v[L].astype(BF)
            self.cp(0).start()
            self.cp(2).start()
        elif step == 1:
            self.S1[1] = v[T].astype(BF)
            self.cp(1).start()
            self.PD[step, L, :] = v[L]
        elif step == 2:
            self.S3[1] = v[L].astype(BF)
            self.cp(3).start()
            self.PD[step, T, :] = v[T]
        else:
            self.PD[0] = v

    def quarter(self):
        self.cp(0).wait_recv()
        self.cp(2).wait_send()
        self.S3[0] = (self.PD[2, self.top, :] + self.R1[0].astype(F32)).astype(BF)
        self.cp(5).start()
        self.cp(2).wait_recv()
        self.cp(0).wait_send()
        self.S1[0] = (self.PD[1, self.low, :] + self.R3[0].astype(F32)).astype(BF)
        self.cp(4).start()

    def finish(self, layer):
        for which in (1, 3, 4, 5):
            self.cp(which).wait_recv()
        for part, R, Q in ((self.top, self.R1, self.Q3), (self.low, self.R3, self.Q1)):
            g = (self.PD[0, part, :] + R[1].astype(F32) + Q[...].astype(F32)).astype(BF)
            self.GD[layer, part, :] = g
            self.SQ[...] += squares(g)
        self.swap(3).wait_send()
        for which in (1, 3, 4, 5):
            self.cp(which).wait_send()


def first_kernel(a0_ref, dh1_ref, dy_ref, act1_ref, wd0_ref, g0_ref, u0_ref, sq1_ref, gg_in, gu_in,
                 gg_ref, gu_ref, gd_ref, sq_ref,
                 A, DH, WD, ACT, DGU, GT, UT, G, GD, SQ, SQD, TS, TR, local, tsem, gsem, xsem, *scatter):
    T, D = A.shape
    F, TM, n = ACT.shape[1], GT.shape[1], TR.shape[0]
    r, rd, nf, tiles = D // n, F // n, F // CH, T // TM
    split = Scatter.scratch(r)
    s = Scatter(r, scatter[: len(split)], G, SQ, (gg_ref.at[0], gu_ref.at[0]), gsem)
    d = DownScatter(rd, scatter[len(split) :], GD, SQD)
    keep = Local(local)
    dy_in = keep(dy_ref, DH)

    def act_in(step):
        return pltpu.make_async_copy(act1_ref.at[:, d.columns(step)], ACT.at[:, d.columns(step)], tsem.at[2, step])

    for step in range(4):
        act_in(step).start()
    def dh_in(t):
        return pltpu.make_async_copy(dh1_ref.at[tile(t, TM), :], DH.at[tile(t, TM), :], tsem.at[3, t])

    later = [keep(wd0_ref, WD), keep(a0_ref, A)]
    others = [lax.rem(s.me + i, n) for i in range(1, n)]
    meet(others)
    SQ[...] = jnp.zeros_like(SQ)
    SQD[...] = jnp.zeros_like(SQD)

    def fetch(i):
        where = (tile(i % tiles, TM), tile(i // tiles, CH))
        return [pltpu.make_async_copy(ref.at[where], to.at[i % 2], tsem.at[j, i % 2]) for j, (ref, to) in enumerate(((g0_ref, GT), (u0_ref, UT)))]

    for c in fetch(0):
        c.start()
    dy_in.wait()

    @pl.loop(0, 4)
    def _(step):
        act_in(step).wait()
        d.compute(step, ACT, DH)
        for j in range(3):
            when(step == j + 1, lambda: d.halve(j))

    for t in range(tiles):
        dh_in(t).start()
    for c in later:
        c.wait()

    @pl.loop(0, nf)
    def _(f):
        cols = tile(f, CH)

        @pl.loop(0, tiles)
        def _(t):
            i = f * tiles + t

            @pl.when(i + 1 < nf * tiles)
            def _():
                for c in fetch(i + 1):
                    c.start()

            when((t == 0) & (f > 1), lambda: s.quarter(f - 2))
            when((t == 2) & (f > 0), lambda: s.halve(f - 1))
            when((t == 2) & (f == 0), lambda: d.halve(3), d.quarter)
            when(f == 0, dh_in(t).wait)
            for c in fetch(i):
                c.wait()
            for j in range(TM // SUB):
                rows, part = tile(t * (TM // SUB) + j, SUB), pl.ds(j * SUB, SUB)
                dact = nt(DH[rows, :], WD[cols, :]).astype(BF)
                ACT[rows, cols], DGU[rows, :CH], DGU[rows, CH:] = swiglu_back(GT[i % 2, part, :], UT[i % 2, part, :], dact)

        when(f > 1, lambda: s.finish(f - 2))
        s.dot_and_send(f, A[...], DGU[...])
        when(f == 1, lambda: d.finish(1))

    s.quarter(nf - 2)

    @pl.loop(0, 4)
    def _(step):
        d.compute(step, ACT, DH)
        when(step == 0, lambda: s.halve(nf - 1))
        when(step == 1, lambda: s.finish(nf - 2), lambda: d.halve(0))
        when(step == 2, lambda: d.halve(1), lambda: s.quarter(nf - 1))
        when(step == 3, lambda: d.halve(2))

    d.halve(3)
    d.quarter()
    s.finish(nf - 1)
    d.finish(0)
    out = keep(GD, gd_ref)
    TS[...] = jnp.full(TS.shape, jnp.sum(SQ[...]) + jnp.sum(SQD[...]), F32) + sq1_ref[...]
    sums = [remote(TS, TR.at[s.me], xsem.at[0, i], xsem.at[1, s.me], dev) for i, dev in enumerate(others)]
    for c in sums:
        c.start()
    TR[s.me] = TS[...]
    for dev in others:
        remote(TS, TR.at[dev], xsem.at[0, 0], xsem.at[1, dev], others[0]).wait_recv()
    total = TR[0]
    for i in range(1, n):
        total = total + TR[i]
    sq_ref[...] = total
    s.drain(nf - 1)
    for c in sums:
        c.wait_send()
    out.wait()


def adamw(w, m, v, g):
    m = 0.9 * m + 0.1 * g
    v = 0.95 * v + 0.05 * g * g
    step = m * lax.rsqrt(v + 1e-8) + 0.1 * w
    return (w - 0.02 * step).astype(BF), m, v


def solution(mesh):
    n = mesh.shape["dp"]
    ANY, VM = pl.BlockSpec(memory_space=pl.ANY), pl.BlockSpec(memory_space=pltpu.VMEM)
    DMA = pltpu.SemaphoreType.DMA

    def V(*shape, dtype=BF):
        return pltpu.VMEM(shape, dtype)

    def call(body, number, ins, outs, scratch, aliases):
        spec = lambda a: VM if a.shape == (8, 128) else ANY
        return pl.pallas_call(
            body,
            out_shape=outs,
            in_specs=[spec(a) for a in ins],
            out_specs=[spec(a) for a in outs],
            scratch_shapes=scratch,
            input_output_aliases=aliases,
            compiler_params=pltpu.CompilerParams(collective_id=number, has_side_effects=True, vmem_limit_bytes=VMEM_LIMIT),
            name=body.__name__,
        )(*ins)

    def step(x, dy, *arrays):
        (wg, wu, wd), ms, vs = (arrays[i : i + 3] for i in (0, 3, 6))
        x, dy = x[0], dy[0]
        T, D = x.shape
        r, F = wg.shape[1:]
        rd, nf = wd.shape[1], F // CH
        like = jax.ShapeDtypeStruct
        tokens, hidden, wide, down = like((T, D), BF), like((T, F), BF), like((T, F), F32), like((F, D), BF)
        rows, sums = like(wg.shape, BF), like((8, 128), F32)
        TD, DF, FD, TF = V(T, D), V(D, 2 * F), V(F, D), V(T, F)
        gathers = [DMA((2 * nf + 4, 9))] * 2
        G, SQ = V(2, 2, r, CH), V(8, CH, dtype=F32)
        stage = lambda size: [V(2, size, CH, dtype=F32)] * 2
        h1, a0, g0, u0, wd0, wd1 = call(
            forward_kernel, 0, (x, wg, wu, wd), [tokens, tokens, wide, wide, down, down],
            [TD, TD, TF, DF, FD, *stage(CH), DMA((2 * nf + 9,)), DMA((2, 2)), *gathers], {},
        )
        gg, gu, act1, dh1, sq1 = call(
            last_kernel, 1, (h1, dy, wg, wu, wd1), [rows, rows, hidden, tokens, sums],
            [TD, TD, DF, FD, V(T, 2 * F), V(T, CH), G, SQ, DMA((2 * nf + 9,)), DMA((1,)), DMA((2, 2)), *gathers, *Scatter.scratch(r)], {},
        )
        gg, gu, gd, sq = call(
            first_kernel, 2, (a0, dh1, dy, act1, wd0, g0, u0, sq1, gg, gu), [rows, rows, like(wd.shape, BF), sums],
            [TD, TD, FD, TF, V(T, 2 * CH), *stage(CH), G, V(2, rd, D), SQ, V(8, D, dtype=F32), V(8, 128, dtype=F32), V(n, 8, 128, dtype=F32),
             DMA((9,)), DMA((4, 4)), DMA((2, 2)), DMA((2, n)), *Scatter.scratch(r), *DownScatter.scratch(rd, D)],
            {8: 0, 9: 1},
        )
        count = n * (gg.size + gu.size + gd.size)
        factor = jnp.minimum(1.0, 0.5 * lax.rsqrt(sq[0, 0] / count + 1e-30))
        new = [
            adamw(w.astype(F32), m, v, g.astype(F32) * factor)
            for w, m, v, g in zip((wg, wu, wd), ms, vs, (gg, gu, gd), strict=True)
        ]
        return tuple(one[which] for which in range(3) for one in new)

    states, cut = P(("rep", "dp"), None, None), P(None, "dp", None)
    return jax.shard_map(
        step,
        mesh=mesh,
        in_specs=(states, states) + (cut,) * 9,
        out_specs=(P("rep", "dp", None),) * 9,
        check_vma=False,
    )
```

```python
import functools

import jax
import jax.numpy as jnp
from jax import lax
from jax.experimental import pallas as pl
from jax.experimental.pallas import tpu as pltpu
from jax.sharding import PartitionSpec as P

MESH = pl.DeviceIdType.MESH
BF, F32 = jnp.bfloat16, jnp.float32
CH = 512
SUB = 256
VMEM_LIMIT = 67_043_328
FIRST, SECOND, ALL = 0, 1, None


def dot(a, b, ca, cb):
    return lax.dot_general(a, b, (((ca,), (cb,)), ((), ())), preferred_element_type=F32)


nn = functools.partial(dot, ca=1, cb=0)
nt = functools.partial(dot, ca=1, cb=1)
tn = functools.partial(dot, ca=0, cb=0)


def place():
    me = lax.axis_index("dp")
    x, k = me // 2, me % 2
    chips = (x, x + 1 - 2 * (x % 2), (x + 2) % 4, 3 - x)
    return me, k, chips, [2 * c + k for c in chips], [2 * c + 1 - k for c in chips]


def meet(devices):
    barrier = pltpu.get_barrier_semaphore()
    for d in devices:
        pl.semaphore_signal(barrier, device_id={"dp": d}, device_id_type=MESH)
    pl.semaphore_wait(barrier, len(devices))


def remote(src, dst, send, recv, device):
    return pltpu.make_async_remote_copy(src_ref=src, dst_ref=dst, send_sem=send, recv_sem=recv, device_id={"dp": device}, device_id_type=MESH)


def when(condition, *acts):
    @pl.when(condition)
    def _():
        for act in acts:
            act()


def tile(t, size):
    return pl.ds(pl.multiple_of(t * size, size), size)


def lanes(start, size):
    return pl.ds(start if isinstance(start, int) else pl.multiple_of(start, 128), size)


class Local:
    def __init__(self, sems):
        self.sems, self.used = sems, 0

    def __call__(self, src, dst):
        copy = pltpu.make_async_copy(src, dst, self.sems.at[self.used])
        self.used += 1
        copy.start()
        return copy


def normed(h):
    wide = h.astype(F32)
    scale = lax.rsqrt(jnp.mean(wide * wide, -1, keepdims=True) + 1e-6)
    return (wide * scale).astype(BF)


def norm_rows(src, dst):
    @pl.loop(0, src.shape[0] // SUB)
    def _(t):
        dst[tile(t, SUB), :] = normed(src[tile(t, SUB), :])


def squares(g):
    g = g.astype(F32)
    return jnp.sum((g * g).reshape(-1, 8, g.shape[-1]), 0)


class Gather:
    def __init__(self, send, recv):
        self.send, self.recv = send, recv
        self.me, k, chips, (n0, n1, n2, n3), (o0, o1, o2, o3) = place()
        self.partners = (n1, n3, o0)
        self.moves = [
            (n0, ALL, n1), (n0, ALL, n3), (n0, ALL, o0), (n1, FIRST, n3), (n3, SECOND, n1),
            (n1, ALL, o0), (n3, ALL, o0), (n2, FIRST, o0), (n2, SECOND, o0),
        ]
        self.lands = [(n1, ALL), (n3, ALL), (o0, ALL), (n2, FIRST), (n2, SECOND), (o1, ALL), (o3, ALL), (o2, FIRST), (o2, SECOND)]

    def region(self, item, dev, half):
        src, layer, at, buf, blk, r0, rn, c0, cn, by_rows = item
        row = dev * blk + r0
        if half is not ALL:
            if by_rows:
                rn //= 2
                row = row + half * rn
            else:
                cn //= 2
                c0 = c0 + half * cn
        return buf.at[pl.ds(pl.multiple_of(row, 16), rn), lanes(c0, cn)]

    def nth(self, i, item, c):
        source, half, to = self.moves[c]
        src = dst = self.region(item, source, half)
        if source is self.moves[0][0]:
            array, layer, at, buf, blk, r0, rn, c0, cn, by_rows = item
            src = array.at[layer, pl.ds(r0, rn), lanes(at, cn)]
        return remote(src, dst, self.send.at[i, c], self.recv.at[i, c], to)

    def arrived(self, i, item, c):
        what = self.region(item, *self.lands[c])
        remote(what, what, self.send.at[i, c], self.recv.at[i, c], self.partners[0]).wait_recv()

    def issue(self, piece):
        for i, item in piece:
            for c in (0, 1, 2):
                self.nth(i, item, c).start()

    def forward(self, piece):
        for i, item in piece:
            for c in (0, 1):
                self.arrived(i, item, c)
                self.nth(i, item, c + 3).start()
                self.nth(i, item, c + 5).start()

    def pass_on(self, piece):
        for i, item in piece:
            for c in (3, 4):
                self.arrived(i, item, c)
                self.nth(i, item, c + 4).start()

    def complete(self, piece):
        for i, item in piece:
            for c in (2, 5, 6, 7, 8):
                self.arrived(i, item, c)

    def sent(self, piece):
        for i, item in piece:
            for c in range(len(self.moves)):
                self.nth(i, item, c).wait_send()


def pair(layer, r, weights, W, f):
    return [(2 * f + m, (w, layer, f * CH, W, r, 0, r, (2 * f + m) * CH, CH, False)) for m, w in enumerate(weights)]


def own_rows(keep, layer, r, weights, W, me):
    nf = W.shape[1] // (2 * CH)
    return [keep(w.at[layer, :, pl.ds(f * CH, CH)], W.at[tile(me, r), pl.ds((2 * f + m) * CH, CH)]) for m, w in enumerate(weights) for f in range(nf)]


def forward_kernel(x_ref, wg_ref, wu_ref, wd_ref, h1_ref, a1_ref, a0_ref, g0_ref, u0_ref, wd0_ref, wd1_ref,
                   X, A, ACT, W, WD, GS, US, local, save, tiled, send, recv):
    T, D = X.shape
    F = ACT.shape[1]
    TM = GS.shape[1]
    r, rd, nf, tiles = wg_ref.shape[1], wd_ref.shape[1], F // CH, T // TM
    g, keep = Gather(send, recv), Local(local)
    x_in = keep(x_ref, X)
    own = own_rows(keep, 0, r, (wg_ref, wu_ref), W, g.me)
    own += [keep(wd_ref.at[layer], to.at[tile(g.me, rd), :]) for layer, to in enumerate((WD, wd1_ref))]
    meet(g.partners)
    chunk = functools.partial(pair, 0, r, (wg_ref, wu_ref), W)
    rest = [
        [(2 * (nf + layer) + i, (wd_ref, layer, 0, buf, rd, i * (rd // 2), rd // 2, 0, D, True))]
        for layer, buf in enumerate((WD, wd1_ref)) for i in range(2)
    ]

    def on(act, p, condition=True):
        when(condition & (p < nf), lambda: act(chunk(p)))
        for i, piece in enumerate(rest):
            when(condition & (p == nf + i), lambda: act(piece))

    ahead = 2
    for p in range(ahead):
        g.issue(chunk(p))
    x_in.wait()
    norm_rows(X, A)
    out = [keep(A, a0_ref), own.pop()]
    for c in own:
        c.wait()
    for p in range(ahead):
        g.forward(chunk(p))
        g.issue(chunk(p + ahead))
    g.pass_on(chunk(0))

    def saving(f, t):
        rows, cols, slot = tile(t, TM), tile(f, CH), t % 2
        return [pltpu.make_async_copy(S.at[slot], ref.at[rows, cols], save.at[i, slot]) for i, (S, ref) in enumerate(((GS, g0_ref), (US, u0_ref)))]

    @pl.loop(0, nf)
    def _(f):
        g.complete(chunk(f))

        @pl.loop(0, tiles)
        def _(t):
            on(g.forward, f + 2, t == tiles // 2)
            on(g.issue, f + 4, t == tiles // 2)
            copies, slot = saving(f, t), t % 2
            when((t > 1) | (f > 0), *[c.wait for c in copies])
            for j in range(TM // SUB):
                rows, part = tile(t * (TM // SUB) + j, SUB), pl.ds(j * SUB, SUB)
                both = nn(A[rows, :], W[:, tile(f, 2 * CH)])
                gate, up = both[:, :CH], both[:, CH:]
                GS[slot, part, :] = gate
                US[slot, part, :] = up
                ACT[rows, tile(f, CH)] = (gate * jax.nn.sigmoid(gate) * up).astype(BF)
            for c in copies:
                c.start()

        on(g.pass_on, f + 1)

    first, below, *last = rest
    g.complete(first)
    g.forward(last[0])
    g.pass_on(below)
    g.complete(below)
    out.append(keep(WD, wd0_ref))
    out.pop(0).wait()

    def h_out(t):
        rows = tile(t, CH)
        return [pltpu.make_async_copy(S.at[rows, :], ref.at[rows, :], tiled.at[i, t]) for i, (S, ref) in enumerate(((X, h1_ref), (A, a1_ref)))]

    @pl.loop(0, T // CH)
    def _(t):
        rows = tile(t, CH)
        X[rows, :] = (X[rows, :].astype(F32) + nn(ACT[rows, :], WD[...]).astype(BF).astype(F32)).astype(BF)
        A[rows, :] = normed(X[rows, :])
        for c in h_out(t):
            c.start()
        when(t == 0, lambda: g.forward(last[1]))
        when(t == 1, lambda: g.pass_on(last[0]))
        when(t == 2, lambda: g.pass_on(last[1]))

    for p in last:
        g.complete(p)
    for p in [chunk(f) for f in range(nf)] + rest:
        g.sent(p)
    for t in range(tiles - 2, tiles):
        out += saving(nf - 1, t)
    for t in range(T // CH):
        out += h_out(t)
    for c in out:
        c.wait()


class Scatter:
    def __init__(self, r, refs, G, SQ, outs, sems):
        self.outs, self.saves = outs, sems
        self.R, (self.DS, self.DR), (self.AS, self.AR), (self.BS, self.BR), (self.CS, self.CR), (self.ES, self.ER) = refs[0], *zip(refs[2:-1:2], refs[3:-1:2])
        self.Z = refs[1]
        self.r, self.sems, self.G, self.SQ = r, refs[-1], G, SQ
        self.me, self.k, self.chips, (n0, n1, n2, n3), (o0, *_) = place()
        self.routes = ((self.DS, self.DR, o0), (self.AS, self.AR, n1), (self.BS, self.BR, n3), (self.CS, self.CR, n3), (self.ES, self.ER, n1))

    @staticmethod
    def scratch(r):
        sent = [(4, r, 2 * CH), (2, r, CH), (2, r, CH), (r, CH), (r, CH)]
        shapes = [s for one in sent for s in (one, (2, *one))]
        return [pltpu.VMEM((2, 8 * r, 2 * CH), F32), pltpu.VMEM((r, 2 * CH), F32), *[pltpu.VMEM(s, BF) for s in shapes], pltpu.SemaphoreType.DMA((5, 3))]

    def cp(self, which, f):
        src, dst, dev = self.routes[which]
        return remote(src, dst.at[f % 2], self.sems.at[which, 0], self.sems.at[which, 1 + f % 2], dev)

    def rows(self, q, core):
        return pl.ds(pl.multiple_of((2 * self.chips[q] + core) * self.r, 16), self.r)

    def dot_and_send(self, f, a, b):
        R = self.R.at[f % 2]
        R[...] = tn(a, b)
        when(f > 0, self.cp(0, f).wait_send)
        for q in range(4):
            self.DS[q] = R[self.rows(q, 1 - self.k), :].astype(BF)
        self.cp(0, f).start()

    def halve(self, f):
        s, R = f % 2, self.R.at[f % 2]
        self.cp(0, f).wait_recv()
        when(f > 0, self.cp(1, f).wait_send, self.cp(2, f).wait_send)
        v = [R[self.rows(q, self.k), :] + self.DR[s, q].astype(F32) for q in range(4)]
        self.AS[0], self.AS[1] = v[1][:, :CH].astype(BF), v[2][:, :CH].astype(BF)
        self.BS[0], self.BS[1] = v[3][:, CH:].astype(BF), v[2][:, CH:].astype(BF)
        R[self.rows(0, self.k), :] = v[0]
        R[self.rows(1, self.k), CH:] = v[1][:, CH:]
        R[self.rows(3, self.k), :CH] = v[3][:, :CH]
        self.cp(1, f).start()
        self.cp(2, f).start()

    def quarter(self, f):
        s, R, mine = f % 2, self.R.at[f % 2], self.rows(0, self.k)
        for which in (1, 2):
            self.cp(which, f).wait_recv()
        when(f > 0, self.cp(3, f).wait_send, self.cp(4, f).wait_send)
        self.CS[...] = (R[self.rows(3, self.k), :CH] + self.AR[s, 1].astype(F32)).astype(BF)
        self.ES[...] = (R[self.rows(1, self.k), CH:] + self.BR[s, 1].astype(F32)).astype(BF)
        self.Z[:, :CH] = R[mine, :CH] + self.AR[s, 0].astype(F32)
        self.Z[:, CH:] = R[mine, CH:] + self.BR[s, 0].astype(F32)
        self.cp(3, f).start()
        self.cp(4, f).start()

    def finish(self, f):
        s = f % 2
        for which in (3, 4):
            self.cp(which, f).wait_recv()
        for m, (part, last) in enumerate(((self.Z[:, :CH], self.CR), (self.Z[:, CH:], self.ER))):
            g = (part + last[s].astype(F32)).astype(BF)
            when(f > 1, self.saving(f, m).wait)
            self.G[s, m] = g
            self.saving(f, m).start()
            self.SQ[...] += squares(g)

    def saving(self, f, m):
        return pltpu.make_async_copy(self.G.at[f % 2, m], self.outs[m].at[:, tile(f, CH)], self.saves.at[m, f % 2])

    def drain(self, f):
        for which in range(len(self.routes)):
            self.cp(which, f).wait_send()
        for m in range(2):
            self.saving(f, m).wait()
            self.saving(f - 1, m).wait()


def swiglu_back(gate, up, dact):
    sig = jax.nn.sigmoid(gate)
    silu = gate * sig
    dact = dact.astype(F32)
    return (silu * up).astype(BF), (dact * up * (sig + silu * (1.0 - sig))).astype(BF), (dact * silu).astype(BF)


def last_kernel(h1_ref, a1_ref, dy_ref, wg_ref, wu_ref, wd1_ref, gg_ref, gu_ref, act1_ref, dh1_ref, sq_ref,
                A, DY, W, WD, DGU, ACT, G, SQ, local, save, gsem, send, recv, *scatter):
    T, D = A.shape
    F = W.shape[1] // 2
    TM = 4 * SUB
    r, nf, tiles = wg_ref.shape[1], F // CH, T // TM
    g, keep = Gather(send, recv), Local(local)
    s = Scatter(r, scatter, G, SQ, (gg_ref.at[1], gu_ref.at[1]), gsem)
    first = [keep(dy_ref, DY), keep(wd1_ref, WD)]
    own = [keep(a1_ref, A)] + own_rows(keep, 1, r, (wg_ref, wu_ref), W, g.me)
    meet(g.partners)
    piece = functools.partial(pair, 1, r, (wg_ref, wu_ref), W)
    g.issue(piece(0))
    SQ[...] = jnp.zeros_like(SQ)
    for c in first:
        c.wait()

    @pl.loop(0, T // CH)
    def _(t):
        rows = tile(t, CH)
        dact = nt(DY[rows, :], WD[...]).astype(BF)
        for f in range(nf):
            DGU[rows, pl.ds((2 * f + 1) * CH, CH)] = dact[:, f * CH : (f + 1) * CH]
        when(t == 0, lambda: g.forward(piece(0)), lambda: g.issue(piece(1)))
        when(t == 1, lambda: g.issue(piece(2)))
        when(t == 2, lambda: g.pass_on(piece(0)))

    for c in own:
        c.wait()

    def save_act(f):
        return pltpu.make_async_copy(ACT, act1_ref.at[:, tile(f, CH)], save.at[0])

    @pl.loop(0, nf)
    def _(f):
        cols = tile(f, 2 * CH)
        g.complete(piece(f))
        when(f > 0, lambda: save_act(f).wait())

        @pl.loop(0, tiles)
        def _(t):
            when((t == 0) & (f + 1 < nf), lambda: g.forward(piece(f + 1)))
            when((t == 0) & (f + 3 < nf), lambda: g.issue(piece(f + 3)))
            when((t == 1) & (f > 0), lambda: s.halve(f - 1))
            for j in range(TM // SUB):
                rows = tile(t * (TM // SUB) + j, SUB)
                both = nn(A[rows, :], W[:, cols])
                ACT[rows, :], DGU[rows, tile(2 * f, CH)], DGU[rows, tile(2 * f + 1, CH)] = swiglu_back(both[:, :CH], both[:, CH:], DGU[rows, tile(2 * f + 1, CH)])

        save_act(f).start()
        when(f + 1 < nf, lambda: g.pass_on(piece(f + 1)))
        when(f > 1, lambda: s.quarter(f - 2))
        s.dot_and_send(f, A[...], DGU[:, cols])
        when(f > 1, lambda: s.finish(f - 2))

    save_act(nf - 1).wait()
    keep(h1_ref, A).wait()

    def dh_out(t):
        return pltpu.make_async_copy(DY.at[tile(t, CH), :], dh1_ref.at[tile(t, CH), :], save.at[1 + t])

    @pl.loop(0, T // CH)
    def _(t):
        rows = tile(t, CH)
        da = nt(DGU[rows, :], W[...]).astype(BF).astype(F32)
        wide = A[rows, :].astype(F32)
        scale = lax.rsqrt(jnp.mean(wide * wide, -1, keepdims=True) + 1e-6)
        back = (da * scale - wide * (scale * scale * scale * jnp.mean(da * wide, -1, keepdims=True))).astype(BF)
        DY[rows, :] = (DY[rows, :].astype(F32) + back.astype(F32)).astype(BF)
        dh_out(t).start()
        when(t == 0, lambda: s.quarter(nf - 2), lambda: s.halve(nf - 1))
        when(t == 1, lambda: s.finish(nf - 2))
        when(t == 2, lambda: s.quarter(nf - 1))
        when(t == 3, lambda: s.finish(nf - 1))

    sq_ref[...] = jnp.full(sq_ref.shape, jnp.sum(SQ[...]), F32)
    for f in range(nf):
        g.sent(piece(f))
    s.drain(nf - 1)
    for t in range(T // CH):
        dh_out(t).wait()


class DownScatter:
    def __init__(self, rd, refs, GD, SQ):
        (self.PT, self.PD, self.DS, self.DR, self.S1, self.R1, self.S3, self.R3, self.Q1, self.Q3, self.sems) = refs
        self.rd, self.GD, self.SQ = rd, GD, SQ
        self.me, self.k, self.chips, (n0, n1, n2, n3), (self.partner, *_) = place()
        near = ((self.S1, self.R1, n1), (self.S3, self.R3, n3))
        self.routes = [(S.at[i], R.at[i], n) for S, R, n in near for i in range(2)] + [(self.S1.at[0], self.Q1, n1), (self.S3.at[0], self.Q3, n3)]
        h = rd // 2
        self.top, self.low = slice(0, h), slice(h, rd)

    @staticmethod
    def scratch(rd, D):
        V = pltpu.VMEM
        return [
            V((2 * rd, D), F32), V((3, rd, D), F32), V((rd, D), BF), V((4, rd, D), BF),
            *[V((2, rd // 2, D), BF)] * 4, *[V((rd // 2, D), BF)] * 2, pltpu.SemaphoreType.DMA((10, 2)),
        ]

    def columns(self, s):
        x, x1, x2, x3 = self.chips
        c = jnp.where(s == 0, x2, jnp.where(s == 1, x1, jnp.where(s == 2, x3, x)))
        return pl.ds(pl.multiple_of(c * 2 * self.rd, 128), 2 * self.rd)

    def swap(self, s):
        return remote(self.DS, self.DR.at[s], self.sems.at[s, 0], self.sems.at[s, 1], self.partner)

    def cp(self, which):
        src, dst, dev = self.routes[which]
        return remote(src, dst, self.sems.at[4 + which, 0], self.sems.at[4 + which, 1], dev)

    def compute(self, s, act, rhs):
        rd = self.rd
        self.PT[...] = tn(act[:, self.columns(s)], rhs[...])
        when(s > 0, lambda: self.swap(s - 1).wait_send())
        self.PD[s % 3] = self.PT[tile(self.k, rd), :]
        self.DS[...] = self.PT[tile(1 - self.k, rd), :].astype(BF)
        self.swap(s).start()

    def halve(self, step):
        T, L = self.top, self.low
        self.swap(step).wait_recv()
        v = self.PD[step % 3] + self.DR[step].astype(F32)
        if step == 0:
            self.S1[0], self.S3[0] = v[T].astype(BF), v[L].astype(BF)
            self.cp(0).start()
            self.cp(2).start()
        elif step == 1:
            self.S1[1] = v[T].astype(BF)
            self.cp(1).start()
            self.PD[step, L, :] = v[L]
        elif step == 2:
            self.S3[1] = v[L].astype(BF)
            self.cp(3).start()
            self.PD[step, T, :] = v[T]
        else:
            self.PD[0] = v

    def quarter(self):
        self.cp(0).wait_recv()
        self.cp(2).wait_send()
        self.S3[0] = (self.PD[2, self.top, :] + self.R1[0].astype(F32)).astype(BF)
        self.cp(5).start()
        self.cp(2).wait_recv()
        self.cp(0).wait_send()
        self.S1[0] = (self.PD[1, self.low, :] + self.R3[0].astype(F32)).astype(BF)
        self.cp(4).start()

    def finish(self, layer):
        for which in (1, 3, 4, 5):
            self.cp(which).wait_recv()
        for part, R, Q in ((self.top, self.R1, self.Q3), (self.low, self.R3, self.Q1)):
            g = (self.PD[0, part, :] + R[1].astype(F32) + Q[...].astype(F32)).astype(BF)
            self.GD[layer, part, :] = g
            self.SQ[...] += squares(g)
        self.swap(3).wait_send()
        for which in (1, 3, 4, 5):
            self.cp(which).wait_send()


def first_kernel(a0_ref, dh1_ref, dy_ref, act1_ref, wd0_ref, g0_ref, u0_ref, sq1_ref, gg_in, gu_in,
                 gg_ref, gu_ref, gd_ref, sq_ref,
                 A, DH, WD, ACT, DGU, GT, UT, G, GD, SQ, SQD, TS, TR, local, tsem, gsem, xsem, *scatter):
    T, D = A.shape
    F, TM, n = ACT.shape[1], GT.shape[1], TR.shape[0]
    r, rd, nf, tiles = D // n, F // n, F // CH, T // TM
    split = Scatter.scratch(r)
    s = Scatter(r, scatter[: len(split)], G, SQ, (gg_ref.at[0], gu_ref.at[0]), gsem)
    d = DownScatter(rd, scatter[len(split) :], GD, SQD)
    keep = Local(local)
    dy_in = keep(dy_ref, DH)

    def act_in(step):
        return pltpu.make_async_copy(act1_ref.at[:, d.columns(step)], ACT.at[:, d.columns(step)], tsem.at[2, step])

    for step in range(4):
        act_in(step).start()
    def dh_in(t):
        return pltpu.make_async_copy(dh1_ref.at[tile(t, TM), :], DH.at[tile(t, TM), :], tsem.at[3, t])

    later = [keep(wd0_ref, WD), keep(a0_ref, A)]
    others = [lax.rem(s.me + i, n) for i in range(1, n)]
    meet(others)
    SQ[...] = jnp.zeros_like(SQ)
    SQD[...] = jnp.zeros_like(SQD)

    def fetch(i):
        where = (tile(i % tiles, TM), tile(i // tiles, CH))
        return [pltpu.make_async_copy(ref.at[where], to.at[i % 2], tsem.at[j, i % 2]) for j, (ref, to) in enumerate(((g0_ref, GT), (u0_ref, UT)))]

    for c in fetch(0):
        c.start()
    dy_in.wait()

    @pl.loop(0, 4)
    def _(step):
        act_in(step).wait()
        d.compute(step, ACT, DH)
        for j in range(3):
            when(step == j + 1, lambda: d.halve(j))

    for t in range(tiles):
        dh_in(t).start()
    for c in later:
        c.wait()

    @pl.loop(0, nf)
    def _(f):
        cols = tile(f, CH)

        @pl.loop(0, tiles)
        def _(t):
            i = f * tiles + t

            @pl.when(i + 1 < nf * tiles)
            def _():
                for c in fetch(i + 1):
                    c.start()

            when((t == 0) & (f > 1), lambda: s.quarter(f - 2))
            when((t == 2) & (f > 0), lambda: s.halve(f - 1))
            when((t == 2) & (f == 0), lambda: d.halve(3), d.quarter)
            when(f == 0, dh_in(t).wait)
            for c in fetch(i):
                c.wait()
            for j in range(TM // SUB):
                rows, part = tile(t * (TM // SUB) + j, SUB), pl.ds(j * SUB, SUB)
                dact = nt(DH[rows, :], WD[cols, :]).astype(BF)
                ACT[rows, cols], DGU[rows, :CH], DGU[rows, CH:] = swiglu_back(GT[i % 2, part, :], UT[i % 2, part, :], dact)

        when(f > 1, lambda: s.finish(f - 2))
        s.dot_and_send(f, A[...], DGU[...])
        when(f == 1, lambda: d.finish(1))

    s.quarter(nf - 2)

    @pl.loop(0, 4)
    def _(step):
        d.compute(step, ACT, DH)
        when(step == 0, lambda: s.halve(nf - 1))
        when(step == 1, lambda: s.finish(nf - 2), lambda: d.halve(0))
        when(step == 2, lambda: d.halve(1), lambda: s.quarter(nf - 1))
        when(step == 3, lambda: d.halve(2))

    d.halve(3)
    d.quarter()
    s.finish(nf - 1)
    d.finish(0)
    out = keep(GD, gd_ref)
    TS[...] = jnp.full(TS.shape, jnp.sum(SQ[...]) + jnp.sum(SQD[...]), F32) + sq1_ref[...]
    sums = [remote(TS, TR.at[s.me], xsem.at[0, i], xsem.at[1, s.me], dev) for i, dev in enumerate(others)]
    for c in sums:
        c.start()
    TR[s.me] = TS[...]
    for dev in others:
        remote(TS, TR.at[dev], xsem.at[0, 0], xsem.at[1, dev], others[0]).wait_recv()
    total = TR[0]
    for i in range(1, n):
        total = total + TR[i]
    sq_ref[...] = total
    s.drain(nf - 1)
    for c in sums:
        c.wait_send()
    out.wait()


def adamw_kernel(count, sq_ref, *refs):
    factor = jnp.minimum(1.0, 0.5 * lax.rsqrt(sq_ref[:1, :1] / count + 1e-30))
    for i in range(3):
        w, m, v, g, new_w, new_m, new_v = (refs[j][0] if j < 12 else refs[j] for j in range(i, 21, 3))
        w, g = w.astype(F32), g.astype(F32) * factor
        m = 0.9 * m + 0.1 * g
        v = 0.95 * v + 0.05 * g * g
        step = m * lax.rsqrt(v + 1e-8) + 0.1 * w
        new_w[0], new_m[0], new_v[0] = (w - 0.02 * step).astype(BF), m, v


def adamw(sq, count, weights, ms, vs, gradients):
    blocks = 4
    arrays = (*weights, *ms, *vs, *gradients)

    def spec(a):
        layers, rows, cols = a.shape
        if rows < cols // blocks:
            return pl.BlockSpec((1, rows, cols // blocks), lambda i, j: (i, 0, j))
        return pl.BlockSpec((1, rows // blocks, cols), lambda i, j: (i, j, 0))

    return pl.pallas_call(
        functools.partial(adamw_kernel, count),
        grid=(weights[0].shape[0], blocks),
        out_shape=[jax.ShapeDtypeStruct(a.shape, a.dtype) for a in arrays[:9]],
        in_specs=[pl.BlockSpec(sq.shape, lambda i, j: (0, 0)), *map(spec, arrays)],
        out_specs=[*map(spec, arrays[:9])],
        name="adamw",
    )(sq, *arrays)


def solution(mesh):
    n = mesh.shape["dp"]
    ANY, VM = pl.BlockSpec(memory_space=pl.ANY), pl.BlockSpec(memory_space=pltpu.VMEM)
    DMA = pltpu.SemaphoreType.DMA

    def V(*shape, dtype=BF):
        return pltpu.VMEM(shape, dtype)

    def call(body, number, ins, outs, scratch, aliases):
        spec = lambda a: VM if a.shape == (8, 128) else ANY
        return pl.pallas_call(
            body,
            out_shape=outs,
            in_specs=[spec(a) for a in ins],
            out_specs=[spec(a) for a in outs],
            scratch_shapes=scratch,
            input_output_aliases=aliases,
            compiler_params=pltpu.CompilerParams(collective_id=number, has_side_effects=True, vmem_limit_bytes=VMEM_LIMIT),
            name=body.__name__,
        )(*ins)

    def step(x, dy, *arrays):
        (wg, wu, wd), ms, vs = (arrays[i : i + 3] for i in (0, 3, 6))
        x, dy = x[0], dy[0]
        T, D = x.shape
        r, F = wg.shape[1:]
        rd, nf = wd.shape[1], F // CH
        like = jax.ShapeDtypeStruct
        tokens, hidden, wide, down = like((T, D), BF), like((T, F), BF), like((T, F), F32), like((F, D), BF)
        rows, sums = like(wg.shape, BF), like((8, 128), F32)
        TD, DF, FD, TF = V(T, D), V(D, 2 * F), V(F, D), V(T, F)
        gathers = [DMA((2 * nf + 4, 9))] * 2
        G, SQ = V(2, 2, r, CH), V(8, CH, dtype=F32)
        stage = lambda size: [V(2, size, CH, dtype=F32)] * 2
        h1, a1, a0, g0, u0, wd0, wd1 = call(
            forward_kernel, 0, (x, wg, wu, wd), [tokens, tokens, tokens, wide, wide, down, down],
            [TD, TD, TF, DF, FD, *stage(CH), DMA((2 * nf + 9,)), DMA((2, 2)), DMA((2, T // CH)), *gathers], {},
        )
        gg, gu, act1, dh1, sq1 = call(
            last_kernel, 1, (h1, a1, dy, wg, wu, wd1), [rows, rows, hidden, tokens, sums],
            [TD, TD, DF, FD, V(T, 2 * F), V(T, CH), G, SQ, DMA((2 * nf + 9,)), DMA((1 + T // CH,)), DMA((2, 2)), *gathers, *Scatter.scratch(r)], {},
        )
        gg, gu, gd, sq = call(
            first_kernel, 2, (a0, dh1, dy, act1, wd0, g0, u0, sq1, gg, gu), [rows, rows, like(wd.shape, BF), sums],
            [TD, TD, FD, TF, V(T, 2 * CH), *stage(CH), G, V(2, rd, D), SQ, V(8, D, dtype=F32), V(8, 128, dtype=F32), V(n, 8, 128, dtype=F32),
             DMA((9,)), DMA((4, 4)), DMA((2, 2)), DMA((2, n)), *Scatter.scratch(r), *DownScatter.scratch(rd, D)],
            {8: 0, 9: 1},
        )
        return tuple(adamw(sq, n * (gg.size + gu.size + gd.size), (wg, wu, wd), ms, vs, (gg, gu, gd)))

    states, cut = P(("rep", "dp"), None, None), P(None, "dp", None)
    return jax.shard_map(
        step,
        mesh=mesh,
        in_specs=(states, states) + (cut,) * 9,
        out_specs=(P("rep", "dp", None),) * 9,
        check_vma=False,
    )
```
